8 devices in a mesh: dp: 1 (over z), vblk: 2 (over y), vocab: 4 (over x, core).
Axes of the slice: x: 2, y: 2, z: 1, core: 2. Of those that a mesh axis runs over, the one named last changes fastest.
Arguments:
- hidden: bfloat16 [1024, 4096], P('dp')
- w_head: bfloat16 [4096, 32768], P(None, ('vblk', 'vocab'))
- inv_temp: float32 [1024], P('dp')
- target: int32 [1024], P('dp')
Outputs:
- output 1: float32 [1024, 32768], P('dp', ('vblk', 'vocab'))
- output 2: float32 [1024], P('dp')
All inputs are finite; a program needn't handle non-finite values.
Results may differ from the reference program's by a relative error of at most 0.001.
Values are sent between devices in bfloat16 or wider.
A program may use at most 1 GiB of HBM per device.

```python
import math
import jax
import jax.numpy as jnp
from jax import lax

D = 4096
V = 32768
ROWS = 1024


def setup_inputs(seed: int = 0, part: int = 0) -> dict:
    root_key = jax.random.key(seed)
    key_dir, key_w = jax.random.split(root_key, 2)
    key_h, key_shift, key_temp, key_tgt = jax.random.split(jax.random.fold_in(root_key, part), 4)
    direction = jax.random.normal(key_dir, (D,), jnp.float32)
    direction = direction / jnp.sqrt(jnp.sum(direction * direction))

    def weight_block(block_idx):
        col_ids = (block_idx * 128 + jnp.arange(128)).astype(jnp.float32)
        col_gain = 40.0 + jnp.exp(-8.0 * col_ids / V)
        noise_blk = jax.random.normal(jax.random.fold_in(key_w, block_idx), (D, 128), jnp.float32)
        return (noise_blk * (1.5 / math.sqrt(D)) + direction[:, None] * col_gain[None, :]).astype(jnp.bfloat16)

    w_blocks = lax.map(weight_block, jnp.arange(V // 128))
    w_head = jnp.transpose(w_blocks, (1, 0, 2)).reshape(D, V)
    row_shift = jax.random.uniform(key_shift, (ROWS, 1), jnp.float32, 1.5, 3.5)
    hidden = (jax.random.normal(key_h, (ROWS, D), jnp.float32) + row_shift * direction[None, :]).astype(jnp.bfloat16)
    inv_temp = jax.random.uniform(key_temp, (ROWS,), jnp.float32, 0.75, 1.5)
    target = jax.random.randint(key_tgt, (ROWS,), 0, V, jnp.int32)
    target = target.at[0].set(0).at[ROWS - 1].set(V - 1)
    return {"hidden": hidden, "w_head": w_head, "inv_temp": inv_temp, "target": target}


def reference(hidden, w_head, inv_temp, target):
    logits = jnp.dot(hidden, w_head, preferred_element_type=jnp.float32) * inv_temp[:, None]
    row_max = jnp.max(logits, axis=1, keepdims=True)
    exp_val = jnp.exp(logits - row_max)
    prob_row = exp_val / jnp.sum(exp_val, axis=1, keepdims=True)
    cdf_table = jnp.cumsum(prob_row, axis=1)
    picked = jnp.take_along_axis(cdf_table, target[:, None], axis=1)[:, 0]
    return (cdf_table, picked)
```

```python
import functools
import math

import jax
import jax.numpy as jnp
from jax import lax
from jax.experimental import pallas as pl
from jax.experimental.pallas import tpu as pltpu
from jax.sharding import PartitionSpec as P

MESH = pl.DeviceIdType.MESH
VMEM = pl.BlockSpec(memory_space=pltpu.VMEM)
ANY = pl.BlockSpec(memory_space=pl.ANY)
LOG2E = math.log2(math.e)
BLOCK = 512
UNIT = 256
OUT_ROWS = 64
RING = 4


def block_prefix(logits, prefix, stats, block, row0, tau2, rel):
    sub = lax.broadcasted_iota(jnp.int32, (8, 128), 0)
    for s in range(0, UNIT, 128):
        lanes = pl.ds(row0 + s, 128)
        tiles = []
        for t in range(0, BLOCK, 128):
            turned = logits[s : s + 128, t : t + 128].T
            tiles += [turned[i : i + 8] for i in range(0, 128, 8)]
        top = functools.reduce(jnp.maximum, tiles)
        top = jnp.max(top, axis=0, keepdims=True)
        scale = tau2[0:1, lanes]
        where_tgt = rel[0:1, lanes] - block * BLOCK - sub
        carry = None
        hit = jnp.zeros((8, 128), jnp.float32)
        out = []
        for i, tile in enumerate(tiles):
            e = jnp.exp2((tile - top) * scale)
            for k in (1, 2, 4):
                e = e + jnp.where(sub >= k, pltpu.roll(e, k, 0), 0.0)
            if carry is not None:
                e = e + carry
            carry = e[7:8, :]
            hit = jnp.where(where_tgt == 8 * i, e, hit)
            out.append(e)
        here = sub == block
        for q, value in enumerate((top, carry, jnp.sum(hit, axis=0, keepdims=True))):
            stats[q, :, lanes] = jnp.where(here, value, stats[q, :, lanes])
        per = 128 // 8
        for t in range(BLOCK // 128):
            col = jnp.concatenate(out[per * t : per * (t + 1)], axis=0)
            prefix[block, pl.ds(row0 + s, 128), t * 128 : (t + 1) * 128] = col.T


def main_kernel(h_hbm, w_hbm, tau_ref, tgt_ref, prefix, stats, hbuf, wbuf, z0, z1, tau2, rel, hsem, wsem):
    rows = h_hbm.shape[0]
    width = w_hbm.shape[1]
    units = rows // UNIT
    blocks = width // BLOCK
    zs = (z0, z1)
    me = lax.axis_index("vblk") * lax.axis_size("vocab") + lax.axis_index("vocab")

    def w_copy(c):
        cols = pl.ds(pl.multiple_of(c * BLOCK, BLOCK), BLOCK)
        slot = lax.rem(c, 2)
        return pltpu.make_async_copy(w_hbm.at[:, cols], wbuf.at[slot], wsem.at[slot])

    def h_copy(r):
        part = pl.ds(r * UNIT, UNIT)
        return pltpu.make_async_copy(h_hbm.at[part], hbuf.at[part], hsem.at[r])

    h_copy(0).start()
    w_copy(0).start()
    for r in range(1, units):
        h_copy(r).start()
    tau2[...] = tau_ref[...] * LOG2E
    rel[...] = tgt_ref[...] - me * width
    stats[...] = jnp.zeros_like(stats)
    z1[...] = jnp.zeros_like(z1)
    for r in range(units):
        h_copy(r).wait()

    def body(c, _):
        w_copy(c).wait()

        @pl.when(c + 1 < blocks)
        def _():
            w_copy(c + 1).start()

        w = wbuf.at[lax.rem(c, 2)]
        for r in range(units):
            zs[r % 2][...] = jnp.dot(hbuf[r * UNIT : (r + 1) * UNIT, :], w[...], preferred_element_type=jnp.float32)
            before = zs[(r + 1) % 2]
            if r == 0:
                block_prefix(before, prefix, stats, lax.rem(c + blocks - 1, blocks), rows - UNIT, tau2, rel)
            else:
                block_prefix(before, prefix, stats, c, (r - 1) * UNIT, tau2, rel)
        return 0

    lax.fori_loop(0, blocks, body, 0)
    block_prefix(zs[(units - 1) % 2], prefix, stats, blocks - 1, rows - UNIT, tau2, rel)


def sublane_scan(x):
    sub = lax.broadcasted_iota(jnp.int32, x.shape, 0)
    for k in (1, 2, 4):
        x = x + jnp.where(sub >= k, pltpu.roll(x, k, 0), 0.0)
    return x


def exchange_kernel(width, stats, tau_ref, tgt_ref, coef, picked, mine, theirs, send_sem, recv_sem):
    vocab = lax.axis_size("vocab")
    n = lax.axis_size("vblk") * vocab
    me = lax.axis_index("vblk") * vocab + lax.axis_index("vocab")
    rows = stats.shape[2]
    groups = rows // 128

    def device(d):
        k = lax.rem(me + d, n)
        return {"vblk": k // vocab, "vocab": lax.rem(k, vocab)}

    barrier = pltpu.get_barrier_semaphore()
    for d in range(1, n):
        pl.semaphore_signal(barrier, inc=1, device_id=device(d), device_id_type=MESH)

    tau2 = tau_ref[...] * LOG2E
    top = stats[0]
    best = jnp.max(top, axis=0, keepdims=True)
    weight = jnp.exp2((top - best) * tau2)
    mass = stats[1] * weight
    upto = sublane_scan(mass)
    sub = lax.broadcasted_iota(jnp.int32, upto.shape, 0)
    below = jnp.where(sub == 0, 0.0, pltpu.roll(upto, 1, 0))
    total = upto[7:8, :]
    rel = tgt_ref[...] - me * width
    inside = (rel >= sub * BLOCK) & (rel < (sub + 1) * BLOCK)
    at_tgt = jnp.sum(jnp.where(inside, below + stats[2] * weight, 0.0), axis=0, keepdims=True)
    for q, value in enumerate((best, total, at_tgt)):
        for g in range(groups):
            mine[q, g : g + 1, :] = value[:, g * 128 : (g + 1) * 128]
            theirs[me, q, g : g + 1, :] = value[:, g * 128 : (g + 1) * 128]

    pl.semaphore_wait(barrier, n - 1)
    copies = []
    for d in range(1, n):
        copy = pltpu.make_async_remote_copy(
            src_ref=mine,
            dst_ref=theirs.at[me],
            send_sem=send_sem.at[d - 1],
            recv_sem=recv_sem.at[d - 1],
            device_id=device(d),
            device_id_type=MESH,
        )
        copy.start()
        copies.append(copy)
    for copy in copies:
        copy.wait()

    def compact(ref):
        x = ref[...]
        return jnp.concatenate([x[:, g * 128 : (g + 1) * 128] for g in range(groups)], axis=0)

    t2 = compact(tau_ref) * LOG2E
    owner = compact(tgt_ref) // width
    high = functools.reduce(jnp.maximum, [theirs[k, 0] for k in range(n)])
    masses = []
    grand = low = pick = jnp.zeros((groups, 128), jnp.float32)
    for k in range(n):
        factor = jnp.exp2((theirs[k, 0] - high) * t2)
        part = theirs[k, 1] * factor
        grand = grand + part
        low = low + jnp.where(k < me, part, 0.0)
        pick = pick + jnp.where(k < owner, part, 0.0) + theirs[k, 2] * factor
    inverse = 1.0 / grand
    own = jnp.exp2((mine[0] - high) * t2) * inverse
    low = low * inverse
    picked[...] = pick * inverse
    for g in range(groups):
        cols = slice(g * 128, (g + 1) * 128)
        scale = weight[:, cols] * own[g : g + 1, :]
        offset = low[g : g + 1, :] + below[:, cols] * own[g : g + 1, :]
        coef[g * 128 : (g + 1) * 128, 0:16] = jnp.concatenate([scale, offset], axis=0).T


def finish_kernel(prefix, coef, picked, out_hbm, picked_out, ring, sem):
    blocks = prefix.shape[0]
    rows = prefix.shape[1]
    picked_out[...] = picked[...]

    def copy(i, slot):
        part = pl.ds(pl.multiple_of(i * OUT_ROWS, OUT_ROWS), OUT_ROWS)
        return pltpu.make_async_copy(ring.at[slot], out_hbm.at[part], sem.at[slot])

    def body(j, _):
        for slot in range(RING):
            i = j * RING + slot

            @pl.when(j > 0)
            def _():
                copy(i - RING, slot).wait()

            for s in range(0, OUT_ROWS, 8):
                part = pl.ds(pl.multiple_of(i * OUT_ROWS + s, 8), 8)
                c = coef[part, 0:16]
                for b in range(blocks):
                    x = prefix[b, part, :]
                    ring[slot, s : s + 8, b * BLOCK : (b + 1) * BLOCK] = x * c[:, b : b + 1] + c[:, 8 + b : 9 + b]
            copy(i, slot).start()
        return 0

    steps = rows // OUT_ROWS // RING
    lax.fori_loop(0, steps, body, 0)
    for slot in range(RING):
        copy((steps - 1) * RING + slot, slot).wait()


def solution(mesh):
    vocab_axes = ("vblk", "vocab")

    def local_step(hidden, w_head, inv_temp, target):
        rows, depth = hidden.shape
        width = w_head.shape[1]
        blocks = width // BLOCK
        n = mesh.shape["vblk"] * mesh.shape["vocab"]
        tau = inv_temp.reshape(1, rows)
        tgt = target.reshape(1, rows)
        prefix, stats = pl.pallas_call(
            main_kernel,
            out_shape=(
                pltpu.VMEM((blocks, rows, BLOCK), jnp.float32),
                pltpu.VMEM((3, blocks, rows), jnp.float32),
            ),
            in_specs=[ANY, ANY, VMEM, VMEM],
            out_specs=(VMEM, VMEM),
            scratch_shapes=[
                pltpu.VMEM((rows, depth), jnp.bfloat16),
                pltpu.VMEM((2, depth, BLOCK), jnp.bfloat16),
                pltpu.VMEM((UNIT, BLOCK), jnp.float32),
                pltpu.VMEM((UNIT, BLOCK), jnp.float32),
                pltpu.VMEM((1, rows), jnp.float32),
                pltpu.VMEM((1, rows), jnp.int32),
                pltpu.SemaphoreType.DMA((rows // UNIT,)),
                pltpu.SemaphoreType.DMA((2,)),
            ],
            compiler_params=pltpu.CompilerParams(vmem_limit_bytes=44 << 20),
            name="logits_prefix",
        )(hidden, w_head, tau, tgt)
        coef, picked = pl.pallas_call(
            functools.partial(exchange_kernel, width),
            out_shape=(
                pltpu.VMEM((rows, 128), jnp.float32),
                pltpu.VMEM((rows // 128, 128), jnp.float32),
            ),
            in_specs=[VMEM, VMEM, VMEM],
            out_specs=(VMEM, VMEM),
            scratch_shapes=[
                pltpu.VMEM((3, rows // 128, 128), jnp.float32),
                pltpu.VMEM((n, 3, rows // 128, 128), jnp.float32),
                pltpu.SemaphoreType.DMA((n - 1,)),
                pltpu.SemaphoreType.DMA((n - 1,)),
            ],
            compiler_params=pltpu.CompilerParams(
                vmem_limit_bytes=16 << 20, collective_id=0, has_side_effects=True
            ),
            name="exchange",
        )(stats, tau, tgt)
        table, picked = pl.pallas_call(
            finish_kernel,
            out_shape=(
                jax.ShapeDtypeStruct((rows, width), jnp.float32),
                jax.ShapeDtypeStruct((rows // 128, 128), jnp.float32),
            ),
            in_specs=[VMEM, VMEM, VMEM],
            out_specs=(ANY, VMEM),
            scratch_shapes=[
                pltpu.VMEM((RING, OUT_ROWS, width), jnp.float32),
                pltpu.SemaphoreType.DMA((RING,)),
            ],
            compiler_params=pltpu.CompilerParams(vmem_limit_bytes=16 << 20),
            name="finish",
        )(pltpu.with_memory_space_constraint(prefix, pltpu.VMEM), coef, picked)
        return table, picked.reshape(rows)

    return jax.shard_map(
        local_step,
        mesh=mesh,
        in_specs=(P("dp", None), P(None, vocab_axes), P("dp"), P("dp")),
        out_specs=(P("dp", vocab_axes), P("dp")),
        check_vma=False,
    )
```
